256 devices in a mesh: tp: 64 (over y, x, z_hi), col: 4 (over z_lo, core).
Axes of the slice: x: 4, y: 4, z: 8 (z_hi: 4, z_lo: 2; z = z_hi * 2 + z_lo), core: 2. Of those that a mesh axis runs over, the one named last changes fastest.
Arguments:
- gate_in: bfloat16 [1024, 53248], P('col', 'tp'), may hold values from -6 to 6
- up_in: bfloat16 [1024, 53248], P('col', 'tp'), may hold values from -6 to 6
- down_weight: bfloat16 [53248, 16384], P('tp', 'col'), may hold values from -0.02734375 to 0.02734375
- residual: bfloat16 [1024, 16384], P('tp', 'col'), may hold values from -30 to 30
- norm_gain: bfloat16 [16384], P('col'), may hold values from 0.5 to 1.5
Outputs:
- stream: bfloat16 [1024, 16384], P('tp', 'col')
- normed: bfloat16 [1024, 16384], P('tp', 'col')
The draws below stay inside these ranges and needn't reach their ends.
All inputs are finite; a program needn't handle non-finite values.
Results may differ from the reference program's by a relative error of at most 0.0034.
Values may be sent and summed in bfloat16 or wider, within the bound.
No kernel may reach another device: no remote copies, remote signals or barrier semaphores. Data moves between devices by JAX's collectives and lax.ppermute only.
A program may use at most 128 MiB of HBM per device.

```python
import math
import jax
import jax.numpy as jnp
from jax import lax

D = 16384
FF = 53248
TOKENS = 1024


def draw_residual(key, part):
    key_rows = jax.random.fold_in(key, 11)
    key_values = jax.random.fold_in(key, 23)
    row_scale = jnp.exp(jax.random.uniform(key_rows, (TOKENS, 1), jnp.float32, math.log(0.3), math.log(3.0)))
    ramp = jnp.arange(D, dtype=jnp.float32) / (D - 1)
    col_scale = 0.5 * jnp.exp(ramp * math.log(3.0))
    values = jnp.clip(jax.random.normal(key_values, (TOKENS, D), jnp.float32), -4.0, 4.0)
    return (row_scale * col_scale[None, :] * values).astype(jnp.bfloat16)


def levels(stream_key, extent, shards, smallest, high):
    def one(position, parts):
        draws = jax.random.uniform(jax.random.fold_in(jax.random.fold_in(stream_key, 6), position), (parts,), jnp.float32, smallest / len(shards), high / len(shards))
        return jnp.repeat(jnp.exp(draws), extent[position] // parts).reshape((-1,) + (1,) * (len(extent) - position - 1))

    factor_of = one(*shards[0])
    for cut in shards[1:]:
        factor_of = factor_of * one(*cut)
    return factor_of


def noise(key, dims, scale, most, cuts=(), kind=jnp.bfloat16):
    drawn = scale * jax.random.normal(key, dims, jnp.float32)
    if cuts:
        drawn = drawn * levels(key, dims, cuts, -0.22, 0.18)
    return jnp.clip(drawn, -most, most).astype(kind)


def setup_inputs(seed: int = 0) -> dict:
    arg_keys = jax.random.split(jax.random.key(seed), 6)
    return {
        "gate_in": noise(arg_keys[0], (TOKENS, FF), 1.0, 6.0, ((0, 4), (1, 64))),
        "up_in": noise(arg_keys[1], (TOKENS, FF), 1.0, 6.0, ((0, 4), (1, 64))),
        "down_weight": noise(arg_keys[2], (FF, D), FF ** -0.5, 0.02734375, ((0, 64), (1, 4))),
        "residual": draw_residual(jax.random.fold_in(arg_keys[5], 71), 0),
        "norm_gain": jnp.clip(1.0 + 0.1 * jax.random.normal(arg_keys[4], (D,), jnp.float32), 0.5, 1.5).astype(jnp.bfloat16),
    }


def reference(gate_in, up_in, down_weight, residual, norm_gain):
    hidden = (jax.nn.silu(gate_in.astype(jnp.float32)) * up_in.astype(jnp.float32)).astype(jnp.bfloat16)
    branch = jnp.dot(hidden, down_weight, preferred_element_type=jnp.float32)
    summed = residual.astype(jnp.float32) + branch
    mean_square = lax.optimization_barrier(jnp.mean(summed * summed, axis=1, keepdims=True))
    scaled = summed * lax.rsqrt(mean_square + 1e-05) * norm_gain.astype(jnp.float32)[None, :]
    return (summed.astype(jnp.bfloat16), scaled.astype(jnp.bfloat16))
```

```python
import functools

import jax
import jax.numpy as jnp
from jax import lax
from jax.experimental import pallas as pl
from jax.experimental.pallas import tpu as pltpu
from jax.sharding import Mesh
from jax.sharding import PartitionSpec as P

D = 16384
AXES = ("y", "x", "z", "zl", "core")
SIZES = (4, 4, 4, 2, 2)
TP = ("y", "x", "z")
COL = ("zl", "core")
F32 = jnp.float32
BF16 = jnp.bfloat16
MASK = {"a": 1, "b": 3}
CHUNKS = ((1, 2), (0, 3))


def pairs(partner):
    strides, total = [], 1
    for size in reversed(SIZES):
        strides.insert(0, total)
        total *= size
    found = []
    for me in range(total):
        at = [(me // stride) % size for stride, size in zip(strides, SIZES)]
        found.append((me, sum(p * stride for p, stride in zip(partner(*at), strides))))
    return found


def swap(value, partner):
    return lax.ppermute(value, AXES, pairs(partner))


def along(role, kind):
    mask = MASK[kind]

    def partner(y, x, z, zl, core):
        if (role == "u") == (core == 0):
            return y ^ mask, x, z, zl, core
        return y, x ^ mask, z, zl, core

    return partner


def along_z(kind):
    return lambda y, x, z, zl, core: (y, x, z ^ MASK[kind], zl, core)


def other_core(y, x, z, zl, core):
    return y, x, z, zl, core ^ 1


def other_chip(y, x, z, zl, core):
    return y, x, z, zl ^ 1, core


def diagonal(y, x, z, zl, core):
    return y, x, z, zl ^ 1, core ^ 1


def hidden_kernel(where, gate, up, first, second, rows):
    g = gate[...].astype(F32)
    h = jax.nn.silu(g) * up[...].astype(F32)
    rows[...] = h.T
    x, z = where[0], where[1]
    for out, chunk in zip((first, second), CHUNKS):
        for jx in range(4):
            for place, jz in enumerate(chunk):
                start = pl.multiple_of(((x ^ jx) * 4 + (z ^ jz)) * 16, 16)
                to = (jx * 2 + place) * 16
                out[to : to + 16, :] = rows[pl.ds(start, 16), :].astype(BF16)


def hidden_of(where, gate_in, up_in):
    tokens, units = gate_in.shape
    shape = jax.ShapeDtypeStruct((tokens // 2, units), BF16)
    vmem = pl.BlockSpec(memory_space=pltpu.VMEM)
    return pl.pallas_call(
        hidden_kernel,
        out_shape=(shape, shape),
        in_specs=[pl.BlockSpec(memory_space=pltpu.SMEM), vmem, vmem],
        out_specs=(vmem, vmem),
        scratch_shapes=[pltpu.VMEM((tokens, units), F32)],
        cost_estimate=pl.CostEstimate(flops=10 * tokens * units, bytes_accessed=6 * tokens * units, transcendentals=tokens * units),
    )(where, gate_in.T, up_in.T)


def place_of(kind, j):
    low, high = j & 1, (j >> 1) & 1
    return ((low ^ high) << 1) | high if kind == "a" else (high << 1) | (low ^ high)


def product_kernel(kind, tile, where, own, core_peer, chip_peer, diagonal_peer, weight, keep, send, rows):
    shift, core = where[2], where[3]
    for r, ref in enumerate((own, core_peer, chip_peer, diagonal_peer)):
        jy = place_of(kind, r ^ shift)
        for jx in range(4):
            px = place_of(kind, jx)
            place = jnp.where(core == 0, jy * 4 + px, px * 4 + jy)
            rows[pl.ds(pl.multiple_of(place * 32, 32), 32), :] = ref[jx * 32 : jx * 32 + 32, :]
    half = rows.shape[0] // 2

    def step(i, _):
        columns = pl.ds(pl.multiple_of(i * tile, tile), tile)
        part = jnp.dot(rows[...], weight[:, columns], preferred_element_type=F32)
        keep[:, columns] = part[:half]
        send[:, columns] = part[half:].astype(BF16)
        return 0

    lax.fori_loop(0, weight.shape[1] // tile, step, 0)


def product(kind, where, blocks, weight):
    rows, units = blocks[0].shape
    columns = weight.shape[1]
    vmem = pl.BlockSpec(memory_space=pltpu.VMEM)
    return pl.pallas_call(
        functools.partial(product_kernel, kind, 512),
        out_shape=(jax.ShapeDtypeStruct((2 * rows, columns), F32), jax.ShapeDtypeStruct((2 * rows, columns), BF16)),
        in_specs=[pl.BlockSpec(memory_space=pltpu.SMEM)] + [vmem] * 5,
        out_specs=(vmem, vmem),
        scratch_shapes=[pltpu.VMEM((4 * rows, units), BF16)],
        cost_estimate=pl.CostEstimate(flops=8 * rows * units * columns, bytes_accessed=2 * units * columns, transcendentals=0),
    )(where, *blocks, weight)


def reduced(kind, keep, send):
    other = "b" if kind == "a" else "a"
    columns = keep.shape[1]
    got = swap(send, along("u", kind))
    total = (keep + got.astype(F32)).reshape(2, 4, 32, columns)
    got = swap(total[:, 2:].astype(BF16), along("v", kind))
    total = total[:, :2] + got.astype(F32)
    got = swap(total[1].astype(BF16), along("u", other))
    total = total[0] + got.astype(F32)
    got = swap(total[1].astype(BF16), along("v", other))
    return total[0] + got.astype(F32)


def body(gate_in, up_in, down_weight, residual, norm_gain):
    y, x, z = (lax.axis_index(name) for name in TP)
    zl, core = (lax.axis_index(name) for name in COL)
    where = jnp.stack([x, z, (zl * 2 + core) ^ y, core]).astype(jnp.int32)
    halves = jnp.split(down_weight, 2, axis=1)
    results = []
    for own in hidden_of(where, gate_in, up_in):
        core_peer = swap(own, other_core)
        chip_peer = swap(own, other_chip)
        diagonal_peer = swap(chip_peer, other_core)
        blocks = (own, core_peer, chip_peer, diagonal_peer)
        results.append([reduced(kind, *product(kind, where, blocks, half)) for kind, half in zip("ab", halves)])
    away, home = results
    got = swap(jnp.concatenate([part.astype(BF16) for part in away], axis=1), along_z("a"))
    total = jnp.concatenate(home, axis=1) + got.astype(F32)
    got = swap(total[16:].astype(BF16), along_z("b"))
    branch = total[:16] + got.astype(F32)
    summed = residual.astype(F32) + branch
    squares = jnp.sum(summed * summed, axis=1)
    squares = squares + swap(squares, other_core) + swap(squares, other_chip) + swap(squares, diagonal)
    mean_square = squares[:, None] / D
    scaled = summed * lax.rsqrt(mean_square + 1e-05) * norm_gain.astype(F32)[None, :]
    return (summed.astype(BF16), scaled.astype(BF16))


def solution(mesh):
    split = Mesh(mesh.devices.reshape(SIZES), AXES)
    return jax.shard_map(
        body,
        mesh=split,
        in_specs=(P(COL, TP), P(COL, TP), P(TP, COL), P(TP, COL), P(COL)),
        out_specs=(P(TP, COL), P(TP, COL)),
        check_vma=False,
    )
```

```python
import functools

import jax
import jax.numpy as jnp
from jax import lax
from jax.experimental import pallas as pl
from jax.experimental.pallas import tpu as pltpu
from jax.sharding import Mesh
from jax.sharding import PartitionSpec as P

D = 16384
AXES = ("y", "x", "z", "zl", "core")
SIZES = (4, 4, 4, 2, 2)
TP = ("y", "x", "z")
COL = ("zl", "core")
F32 = jnp.float32
BF16 = jnp.bfloat16
VMEM = pl.BlockSpec(memory_space=pltpu.VMEM)
HBM = pl.BlockSpec(memory_space=pltpu.HBM)
MASK = {"a": 1, "b": 3}
OTHER = {"a": "b", "b": "a"}
GROUPS = ((1, 2), (3, 0))
CHUNKS = {"a0": (1, 2), "b0": (3, 2), "a1": (0, 3), "b1": (0, 1)}


def pairs(partner):
    strides, total = [], 1
    for size in reversed(SIZES):
        strides.insert(0, total)
        total *= size
    found = []
    for me in range(total):
        at = [(me // stride) % size for stride, size in zip(strides, SIZES)]
        found.append((me, sum(p * stride for p, stride in zip(partner(*at), strides))))
    return found


def swap(value, partner):
    return lax.ppermute(value, AXES, pairs(partner))


def along(role, kind):
    mask = MASK[kind]

    def partner(y, x, z, zl, core):
        if (role == "u") == (core == 0):
            return y ^ mask, x, z, zl, core
        return y, x ^ mask, z, zl, core

    return partner


def along_z(kind):
    return lambda y, x, z, zl, core: (y, x, z ^ MASK[kind], zl, core)


def other_core(y, x, z, zl, core):
    return y, x, z, zl, core ^ 1


def other_chip(y, x, z, zl, core):
    return y, x, z, zl ^ 1, core


def call(kernel, outs, ins, flops, specs=None, scratch=(), limit=2 << 20):
    return pl.pallas_call(
        kernel,
        out_shape=tuple(jax.ShapeDtypeStruct(shape, dtype) for shape, dtype in outs),
        in_specs=specs or [VMEM] * len(ins),
        out_specs=(VMEM,) * len(outs),
        scratch_shapes=scratch,
        compiler_params=pltpu.CompilerParams(vmem_limit_bytes=limit),
        cost_estimate=pl.CostEstimate(flops=flops, bytes_accessed=1 << 20, transcendentals=0),
    )(*ins)


def spread_kernel(hidden, first, second, rows):
    rows[...] = hidden[...].astype(F32).T
    x, z = lax.axis_index("x"), lax.axis_index("z")
    for out, group in zip((first, second), GROUPS):
        for jx in range(4):
            for place, jz in enumerate(group):
                start = pl.multiple_of(((x ^ jx) * 4 + (z ^ jz)) * 16, 16)
                to = (jx * 2 + place) * 16
                out[to : to + 16, :] = rows[pl.ds(start, 16), :].astype(BF16)


def hidden_of(gate_in, up_in):
    tokens, units = gate_in.shape
    hidden = (jax.nn.silu(gate_in.astype(F32)) * up_in.astype(F32)).astype(BF16)
    half = ((tokens // 2, units), BF16)
    return call(spread_kernel, (half, half), (hidden.T,), 1 << 24, scratch=[pltpu.VMEM((tokens, units), F32)], limit=4 << 20)


def place_of(kind, j):
    low, high = j & 1, (j >> 1) & 1
    return ((low ^ high) << 1) | high if kind == "a" else (high << 1) | (low ^ high)


def send_kernel(kind, sources, tile, *refs):
    *blocks, weight, rows, send = refs
    first = "ab".index(kind) * send.shape[1]
    core = lax.axis_index("core")
    shift = (lax.axis_index("zl") * 2 + core) ^ lax.axis_index("y")
    for r in range(4):
        jy = place_of(kind, r ^ shift)
        for jx in range(4):
            px = place_of(kind, jx)
            place = jnp.where(core == 0, jy * 4 + px, px * 4 + jy) * 32
            for k, (group, index) in enumerate(sources):
                start = (jx * 2 + index) * 16
                to = pl.multiple_of(place + 16 * k, 16)
                rows[pl.ds(to, 16), :] = blocks[group * 4 + r][start : start + 16, :]
    half = send.shape[0]
    for at in range(0, send.shape[1], tile):
        span = slice(at, at + tile)
        there = slice(first + at, first + at + tile)
        send[:, span] = jnp.dot(rows[half:, :], weight[:, there], preferred_element_type=F32).astype(BF16)


def keep_kernel(kind, tile, rows, weight, keep):
    half = keep.shape[0]
    first = "ab".index(kind) * keep.shape[1]
    for at in range(0, keep.shape[1], tile):
        span = slice(at, at + tile)
        there = slice(first + at, first + at + tile)
        keep[:, span] = jnp.dot(rows[:half, :], weight[:, there], preferred_element_type=F32)


def product(part, groups, weight):
    wanted = [next((g, group.index(jz)) for g, group in enumerate(GROUPS) if jz in group) for jz in CHUNKS[part]]
    used = sorted({g for g, _ in wanted})
    blocks = [block for g in used for block in groups[g]]
    sources = [(used.index(g), index) for g, index in wanted]
    rows, units = blocks[0].shape
    columns = weight.shape[1] // 2
    half = 2 * rows
    flops = 4 * rows * units * columns
    placed, send = call(
        functools.partial(send_kernel, part[0], sources, 512),
        (((2 * half, units), BF16), ((half, columns), BF16)),
        (*blocks, weight),
        flops,
    )
    (keep,) = call(functools.partial(keep_kernel, part[0], 512), (((half, columns), F32),), (placed, weight), flops)
    return keep, send


def fetch_kernel(weight, out, sem):
    copy = pltpu.make_async_copy(weight, out, sem)
    copy.start()
    copy.wait()


def fetched(weight):
    return call(
        fetch_kernel,
        ((weight.shape, weight.dtype),),
        (weight,),
        1 << 30,
        specs=[HBM],
        scratch=[pltpu.SemaphoreType.DMA],
        limit=8 << 20,
    )[0]


def add_kernel(groups, keep, got, kept, sent):
    size = keep.shape[0] // groups
    half = size // 2
    for g in range(groups):
        mine, theirs = slice(g * size, g * size + half), slice(g * size + half, (g + 1) * size)
        to = slice(g * half, (g + 1) * half)
        sent[to, :] = (keep[theirs, :] + got[theirs, :].astype(F32)).astype(BF16)
        kept[to, :] = keep[mine, :] + got[mine, :].astype(F32)


def add(groups, keep, got):
    rows, columns = keep.shape
    shape = (rows // 2, columns)
    return call(functools.partial(add_kernel, groups), ((shape, F32), (shape, BF16)), (keep, got), rows * columns)


def away_kernel(keep, got, sent):
    sent[...] = (keep[...] + got[...].astype(F32)).astype(BF16)


def home_kernel(keep, got, more, kept, sent):
    half = kept.shape[0]
    total = keep[...] + got[...].astype(F32) + more[...].astype(F32)
    kept[...] = total[:half]
    sent[...] = total[half:].astype(BF16)


def reduced(part, groups, weight):
    kind = part[0]
    keep, send = product(part, groups, weight)
    steps = ((2, along("u", kind)), (1, along("v", kind)), (1, along("u", OTHER[kind])))
    for count, partner in steps:
        got = swap(send, partner)
        keep, send = add(count, keep, got)
    return keep, swap(send, along("v", OTHER[kind]))


def finish_kernel(keep_a, got_a, keep_b, got_b, residual, summed, squares):
    columns = keep_a.shape[1]
    total = 0.0
    for i, (keep, got) in enumerate(((keep_a, got_a), (keep_b, got_b))):
        here = slice(i * columns, (i + 1) * columns)
        value = residual[:, here].astype(F32) + (keep[...] + got[...].astype(F32))
        summed[:, here] = value
        total = total + jnp.sum(value * value, axis=1, keepdims=True)
    squares[...] = jnp.broadcast_to(total, squares.shape)


def body(gate_in, up_in, down_weight, residual, norm_gain):
    weight = fetched(down_weight)
    groups = []
    for own in hidden_of(gate_in, up_in):
        core_peer = swap(own, other_core)
        chip_peer = swap(own, other_chip)
        groups.append((own, core_peer, chip_peer, swap(chip_peer, other_core)))
    parts = {part: reduced(part, groups, weight) for part in CHUNKS}
    last = []
    for kind in "ab":
        keep, got = parts[kind + "0"]
        rows, columns = keep.shape
        (send,) = call(away_kernel, (((rows, columns), BF16),), (keep, got), rows * columns)
        more = swap(send, along_z(kind))
        half = (rows // 2, columns)
        keep, send = call(home_kernel, ((half, F32), (half, BF16)), (*parts[kind + "1"], more), rows * columns)
        last += [keep, swap(send, along_z(OTHER[kind]))]
    tokens = residual.shape[0]
    summed, squares = call(finish_kernel, ((residual.shape, F32), ((tokens, 128), F32)), (*last, residual), residual.size)
    squares = squares + swap(squares, other_core)
    squares = squares + swap(squares, other_chip)
    mean_square = squares[:, :1] / D
    scaled = summed * lax.rsqrt(mean_square + 1e-05) * norm_gain.astype(F32)[None, :]
    return (summed.astype(BF16), scaled.astype(BF16))


def solution(mesh):
    split = Mesh(mesh.devices.reshape(SIZES), AXES)
    return jax.shard_map(
        body,
        mesh=split,
        in_specs=(P(COL, TP), P(COL, TP), P(TP, COL), P(TP, COL), P(COL)),
        out_specs=(P(TP, COL), P(TP, COL)),
        check_vma=False,
    )
```

```python
import functools

import jax
import jax.numpy as jnp
from jax import lax
from jax.experimental import pallas as pl
from jax.experimental.pallas import tpu as pltpu
from jax.sharding import Mesh
from jax.sharding import PartitionSpec as P

D = 16384
AXES = ("y", "x", "z", "zl", "core")
SIZES = (4, 4, 4, 2, 2)
TP = ("y", "x", "z")
COL = ("zl", "core")
F32 = jnp.float32
BF16 = jnp.bfloat16
VMEM = pl.BlockSpec(memory_space=pltpu.VMEM)
HBM = pl.BlockSpec(memory_space=pltpu.HBM)
MASK = {"a": 1, "b": 3}
OTHER = {"a": "b", "b": "a"}
GROUPS = ((1, 2), (3,), (0,))
CHUNKS = {"a0": (1, 2), "b0": (3, 2), "a1": (0, 3), "b1": (0, 1)}


def pairs(partner):
    strides, total = [], 1
    for size in reversed(SIZES):
        strides.insert(0, total)
        total *= size
    found = []
    for me in range(total):
        at = [(me // stride) % size for stride, size in zip(strides, SIZES)]
        found.append((me, sum(p * stride for p, stride in zip(partner(*at), strides))))
    return found


def swap(value, partner):
    return lax.ppermute(value, AXES, pairs(partner))


def along(role, kind):
    mask = MASK[kind]

    def partner(y, x, z, zl, core):
        if (role == "u") == (core == 0):
            return y ^ mask, x, z, zl, core
        return y, x ^ mask, z, zl, core

    return partner


def along_z(kind):
    return lambda y, x, z, zl, core: (y, x, z ^ MASK[kind], zl, core)


def other_core(y, x, z, zl, core):
    return y, x, z, zl, core ^ 1


def other_chip(y, x, z, zl, core):
    return y, x, z, zl ^ 1, core


def call(kernel, outs, ins, flops, specs=None, scratch=(), limit=2 << 20):
    return pl.pallas_call(
        kernel,
        out_shape=tuple(jax.ShapeDtypeStruct(shape, dtype) for shape, dtype in outs),
        in_specs=specs or [VMEM] * len(ins),
        out_specs=(VMEM,) * len(outs),
        scratch_shapes=scratch,
        compiler_params=pltpu.CompilerParams(vmem_limit_bytes=limit),
        cost_estimate=pl.CostEstimate(flops=flops, bytes_accessed=1 << 20, transcendentals=0),
    )(*ins)


def spread_kernel(hidden, *refs):
    *outs, rows = refs
    rows[...] = hidden[...].astype(F32).T
    x, z = lax.axis_index("x"), lax.axis_index("z")
    for out, group in zip(outs, GROUPS):
        for jx in range(4):
            for place, jz in enumerate(group):
                start = pl.multiple_of(((x ^ jx) * 4 + (z ^ jz)) * 16, 16)
                to = (jx * len(group) + place) * 16
                out[to : to + 16, :] = rows[pl.ds(start, 16), :].astype(BF16)


def hidden_of(gate_in, up_in):
    tokens, units = gate_in.shape
    hidden = (jax.nn.silu(gate_in.astype(F32)) * up_in.astype(F32)).astype(BF16)
    outs = [((tokens // 4 * len(group), units), BF16) for group in GROUPS]
    return call(spread_kernel, outs, (hidden.T,), 1 << 24, scratch=[pltpu.VMEM((tokens, units), F32)], limit=4 << 20)


def place_of(kind, j):
    low, high = j & 1, (j >> 1) & 1
    return ((low ^ high) << 1) | high if kind == "a" else (high << 1) | (low ^ high)


def send_kernel(kind, sources, tile, *refs):
    *blocks, weight, rows, send = refs
    first = "ab".index(kind) * send.shape[1]
    core = lax.axis_index("core")
    shift = (lax.axis_index("zl") * 2 + core) ^ lax.axis_index("y")
    for r in range(4):
        jy = place_of(kind, r ^ shift)
        for jx in range(4):
            px = place_of(kind, jx)
            place = jnp.where(core == 0, jy * 4 + px, px * 4 + jy) * 32
            for k, (group, size, index) in enumerate(sources):
                start = (jx * size + index) * 16
                to = pl.multiple_of(place + 16 * k, 16)
                rows[pl.ds(to, 16), :] = blocks[group * 4 + r][start : start + 16, :]
    half = send.shape[0]
    for at in range(0, send.shape[1], tile):
        span = slice(at, at + tile)
        there = slice(first + at, first + at + tile)
        send[:, span] = jnp.dot(rows[half:, :], weight[:, there], preferred_element_type=F32).astype(BF16)


def keep_kernel(kind, tile, rows, weight, keep):
    half = keep.shape[0]
    first = "ab".index(kind) * keep.shape[1]
    for at in range(0, keep.shape[1], tile):
        span = slice(at, at + tile)
        there = slice(first + at, first + at + tile)
        keep[:, span] = jnp.dot(rows[:half, :], weight[:, there], preferred_element_type=F32)


def product(part, groups, weight):
    wanted = [next((g, group.index(jz)) for g, group in enumerate(GROUPS) if jz in group) for jz in CHUNKS[part]]
    used = sorted({g for g, _ in wanted})
    blocks = [block for g in used for block in groups[g]]
    sources = [(used.index(g), len(GROUPS[g]), index) for g, index in wanted]
    units = weight.shape[0]
    rows = sum(group[0].shape[0] for group in groups) // 2
    columns = weight.shape[1] // 2
    half = 2 * rows
    flops = 4 * rows * units * columns
    placed, send = call(
        functools.partial(send_kernel, part[0], sources, 512),
        (((2 * half, units), BF16), ((half, columns), BF16)),
        (*blocks, weight),
        flops,
    )
    (keep,) = call(functools.partial(keep_kernel, part[0], 512), (((half, columns), F32),), (placed, weight), flops)
    return keep, send


def fetch_kernel(weight, out, sem):
    copy = pltpu.make_async_copy(weight, out, sem)
    copy.start()
    copy.wait()


def fetched(weight):
    return call(
        fetch_kernel,
        ((weight.shape, weight.dtype),),
        (weight,),
        1 << 30,
        specs=[HBM],
        scratch=[pltpu.SemaphoreType.DMA],
        limit=8 << 20,
    )[0]


def add_kernel(groups, keep, got, kept, sent):
    size = keep.shape[0] // groups
    half = size // 2
    for g in range(groups):
        mine, theirs = slice(g * size, g * size + half), slice(g * size + half, (g + 1) * size)
        to = slice(g * half, (g + 1) * half)
        sent[to, :] = (keep[theirs, :] + got[theirs, :].astype(F32)).astype(BF16)
        kept[to, :] = keep[mine, :] + got[mine, :].astype(F32)


def add(groups, keep, got):
    rows, columns = keep.shape
    shape = (rows // 2, columns)
    return call(functools.partial(add_kernel, groups), ((shape, F32), (shape, BF16)), (keep, got), rows * columns)


def away_kernel(keep, got, sent):
    sent[...] = (keep[...] + got[...].astype(F32)).astype(BF16)


def home_kernel(keep, got, more, kept, sent):
    half = kept.shape[0]
    total = keep[...] + got[...].astype(F32) + more[...].astype(F32)
    kept[...] = total[:half]
    sent[...] = total[half:].astype(BF16)


def reduced(part, groups, weight):
    kind = part[0]
    keep, send = product(part, groups, weight)
    steps = ((2, along("u", kind)), (1, along("v", kind)), (1, along("u", OTHER[kind])))
    for count, partner in steps:
        got = swap(send, partner)
        keep, send = add(count, keep, got)
    return keep, swap(send, along("v", OTHER[kind]))


def finish_kernel(keep_a, got_a, keep_b, got_b, residual, summed, squares):
    columns = keep_a.shape[1]
    total = 0.0
    for i, (keep, got) in enumerate(((keep_a, got_a), (keep_b, got_b))):
        here = slice(i * columns, (i + 1) * columns)
        value = residual[:, here].astype(F32) + (keep[...] + got[...].astype(F32))
        summed[:, here] = value
        total = total + jnp.sum(value * value, axis=1, keepdims=True)
    squares[...] = jnp.broadcast_to(total, squares.shape)


def body(gate_in, up_in, down_weight, residual, norm_gain):
    weight = fetched(down_weight)
    groups = []
    for own in hidden_of(gate_in, up_in):
        core_peer = swap(own, other_core)
        chip_peer = swap(own, other_chip)
        groups.append((own, core_peer, chip_peer, swap(chip_peer, other_core)))
    parts = {part: reduced(part, groups, weight) for part in CHUNKS}
    last = []
    for kind in "ab":
        keep, got = parts[kind + "0"]
        rows, columns = keep.shape
        (send,) = call(away_kernel, (((rows, columns), BF16),), (keep, got), rows * columns)
        more = swap(send, along_z(kind))
        half = (rows // 2, columns)
        keep, send = call(home_kernel, ((half, F32), (half, BF16)), (*parts[kind + "1"], more), rows * columns)
        last += [keep, swap(send, along_z(OTHER[kind]))]
    tokens = residual.shape[0]
    summed, squares = call(finish_kernel, ((residual.shape, F32), ((tokens, 128), F32)), (*last, residual), residual.size)
    squares = squares + swap(squares, other_core)
    squares = squares + swap(squares, other_chip)
    mean_square = squares[:, :1] / D
    scaled = summed * lax.rsqrt(mean_square + 1e-05) * norm_gain.astype(F32)[None, :]
    return (summed.astype(BF16), scaled.astype(BF16))


def solution(mesh):
    split = Mesh(mesh.devices.reshape(SIZES), AXES)
    return jax.shard_map(
        body,
        mesh=split,
        in_specs=(P(COL, TP), P(COL, TP), P(TP, COL), P(TP, COL), P(COL)),
        out_specs=(P(TP, COL), P(TP, COL)),
        check_vma=False,
    )
```

```python
import functools

import jax
import jax.numpy as jnp
from jax import lax
from jax.experimental import pallas as pl
from jax.experimental.pallas import tpu as pltpu
from jax.sharding import Mesh
from jax.sharding import PartitionSpec as P

D = 16384
AXES = ("y", "x", "z", "zl", "core")
SIZES = (4, 4, 4, 2, 2)
TP = ("y", "x", "z")
COL = ("zl", "core")
F32 = jnp.float32
BF16 = jnp.bfloat16
VMEM = pl.BlockSpec(memory_space=pltpu.VMEM)
HBM = pl.BlockSpec(memory_space=pltpu.HBM)
MASK = {"a": 1, "b": 3}
OTHER = {"a": "b", "b": "a"}
GROUPS = ((1, 2), (3,), (0,))
CHUNKS = {"a0": (1, 2), "b0": (3, 2), "a1": (0, 3), "b1": (0, 1)}


def pairs(partner):
    strides, total = [], 1
    for size in reversed(SIZES):
        strides.insert(0, total)
        total *= size
    found = []
    for me in range(total):
        at = [(me // stride) % size for stride, size in zip(strides, SIZES)]
        found.append((me, sum(p * stride for p, stride in zip(partner(*at), strides))))
    return found


def swap(value, partner):
    return lax.ppermute(value, AXES, pairs(partner))


def along(role, kind):
    mask = MASK[kind]

    def partner(y, x, z, zl, core):
        if (role == "u") == (core == 0):
            return y ^ mask, x, z, zl, core
        return y, x ^ mask, z, zl, core

    return partner


def along_z(kind):
    return lambda y, x, z, zl, core: (y, x, z ^ MASK[kind], zl, core)


def other_core(y, x, z, zl, core):
    return y, x, z, zl, core ^ 1


def other_chip(y, x, z, zl, core):
    return y, x, z, zl ^ 1, core


def diagonal(y, x, z, zl, core):
    return y, x, z, zl ^ 1, core ^ 1


def call(kernel, outs, ins, flops, specs=None, scratch=(), limit=2 << 20):
    return pl.pallas_call(
        kernel,
        out_shape=tuple(jax.ShapeDtypeStruct(shape, dtype) for shape, dtype in outs),
        in_specs=specs or [VMEM] * len(ins),
        out_specs=(VMEM,) * len(outs),
        scratch_shapes=scratch,
        compiler_params=pltpu.CompilerParams(vmem_limit_bytes=limit),
        cost_estimate=pl.CostEstimate(flops=flops, bytes_accessed=1 << 20, transcendentals=0),
    )(*ins)


def spread_kernel(hidden, *refs):
    *outs, rows = refs
    rows[...] = hidden[...].astype(F32).T
    x, z = lax.axis_index("x"), lax.axis_index("z")
    for out, group in zip(outs, GROUPS):
        for jx in range(4):
            for place, jz in enumerate(group):
                start = pl.multiple_of(((x ^ jx) * 4 + (z ^ jz)) * 16, 16)
                to = (jx * len(group) + place) * 16
                out[to : to + 16, :] = rows[pl.ds(start, 16), :].astype(BF16)


def hidden_of(gate_in, up_in):
    tokens, units = gate_in.shape
    hidden = (jax.nn.silu(gate_in.astype(F32)) * up_in.astype(F32)).astype(BF16)
    outs = [((tokens // 4 * len(group), units), BF16) for group in GROUPS]
    return call(spread_kernel, outs, (hidden.T,), 1 << 24, scratch=[pltpu.VMEM((tokens, units), F32)], limit=4 << 20)


def place_of(kind, j):
    low, high = j & 1, (j >> 1) & 1
    return ((low ^ high) << 1) | high if kind == "a" else (high << 1) | (low ^ high)


def send_kernel(kind, sources, tile, *refs):
    *blocks, weight, rows, send = refs
    first = "ab".index(kind) * send.shape[1]
    core = lax.axis_index("core")
    shift = (lax.axis_index("zl") * 2 + core) ^ lax.axis_index("y")
    for r in range(4):
        jy = place_of(kind, r ^ shift)
        for jx in range(4):
            px = place_of(kind, jx)
            place = jnp.where(core == 0, jy * 4 + px, px * 4 + jy) * 32
            for k, (group, size, index) in enumerate(sources):
                start = (jx * size + index) * 16
                to = pl.multiple_of(place + 16 * k, 16)
                rows[pl.ds(to, 16), :] = blocks[group * 4 + r][start : start + 16, :]
    half = send.shape[0]
    for at in range(0, send.shape[1], tile):
        span = slice(at, at + tile)
        there = slice(first + at, first + at + tile)
        send[:, span] = jnp.dot(rows[half:, :], weight[:, there], preferred_element_type=F32).astype(BF16)


def keep_kernel(kind, tile, rows, weight, keep):
    half = keep.shape[0]
    first = "ab".index(kind) * keep.shape[1]
    for at in range(0, keep.shape[1], tile):
        span = slice(at, at + tile)
        there = slice(first + at, first + at + tile)
        keep[:, span] = jnp.dot(rows[:half, :], weight[:, there], preferred_element_type=F32)


def product(part, groups, weight):
    wanted = [next((g, group.index(jz)) for g, group in enumerate(GROUPS) if jz in group) for jz in CHUNKS[part]]
    used = sorted({g for g, _ in wanted})
    blocks = [block for g in used for block in groups[g]]
    sources = [(used.index(g), len(GROUPS[g]), index) for g, index in wanted]
    units = weight.shape[0]
    rows = sum(group[0].shape[0] for group in groups) // 2
    columns = weight.shape[1] // 2
    half = 2 * rows
    flops = 4 * rows * units * columns
    placed, send = call(
        functools.partial(send_kernel, part[0], sources, 512),
        (((2 * half, units), BF16), ((half, columns), BF16)),
        (*blocks, weight),
        flops,
    )
    (keep,) = call(functools.partial(keep_kernel, part[0], 512), (((half, columns), F32),), (placed, weight), flops)
    return keep, send


def fetch_kernel(weight, out, sem):
    copy = pltpu.make_async_copy(weight, out, sem)
    copy.start()
    copy.wait()


def fetched(weight):
    return call(
        fetch_kernel,
        ((weight.shape, weight.dtype),),
        (weight,),
        1 << 30,
        specs=[HBM],
        scratch=[pltpu.SemaphoreType.DMA],
        limit=8 << 20,
    )[0]


def add_kernel(groups, keep, got, kept, sent):
    size = keep.shape[0] // groups
    half = size // 2
    for g in range(groups):
        mine, theirs = slice(g * size, g * size + half), slice(g * size + half, (g + 1) * size)
        to = slice(g * half, (g + 1) * half)
        sent[to, :] = (keep[theirs, :] + got[theirs, :].astype(F32)).astype(BF16)
        kept[to, :] = keep[mine, :] + got[mine, :].astype(F32)


def add(groups, keep, got):
    rows, columns = keep.shape
    shape = (rows // 2, columns)
    return call(functools.partial(add_kernel, groups), ((shape, F32), (shape, BF16)), (keep, got), rows * columns)


def away_kernel(keep, got, sent):
    sent[...] = (keep[...] + got[...].astype(F32)).astype(BF16)


def home_kernel(keep, got, more, kept, sent):
    half = kept.shape[0]
    total = keep[...] + got[...].astype(F32) + more[...].astype(F32)
    kept[...] = total[:half]
    sent[...] = total[half:].astype(BF16)


def reduced(part, groups, weight):
    kind = part[0]
    keep, send = product(part, groups, weight)
    steps = ((2, along("u", kind)), (1, along("v", kind)), (1, along("u", OTHER[kind])))
    for count, partner in steps:
        got = swap(send, partner)
        keep, send = add(count, keep, got)
    return keep, swap(send, along("v", OTHER[kind]))


def finish_kernel(keep_a, got_a, keep_b, got_b, residual, summed, squares):
    columns = keep_a.shape[1]
    total = 0.0
    for i, (keep, got) in enumerate(((keep_a, got_a), (keep_b, got_b))):
        here = slice(i * columns, (i + 1) * columns)
        value = residual[:, here].astype(F32) + (keep[...] + got[...].astype(F32))
        summed[:, here] = value
        total = total + jnp.sum(value * value, axis=1, keepdims=True)
    squares[...] = jnp.broadcast_to(total, squares.shape)


def body(gate_in, up_in, down_weight, residual, norm_gain):
    weight = fetched(down_weight)
    groups = []
    for own in hidden_of(gate_in, up_in):
        core_peer = swap(own, other_core)
        chip_peer = swap(own, other_chip)
        groups.append((own, core_peer, chip_peer, swap(chip_peer, other_core)))
    parts = {part: reduced(part, groups, weight) for part in CHUNKS}
    last = []
    for kind in "ab":
        keep, got = parts[kind + "0"]
        rows, columns = keep.shape
        (send,) = call(away_kernel, (((rows, columns), BF16),), (keep, got), rows * columns)
        more = swap(send, along_z(kind))
        half = (rows // 2, columns)
        keep, send = call(home_kernel, ((half, F32), (half, BF16)), (*parts[kind + "1"], more), rows * columns)
        last += [keep, swap(send, along_z(OTHER[kind]))]
    tokens = residual.shape[0]
    summed, squares = call(finish_kernel, ((residual.shape, F32), ((tokens, 128), F32)), (*last, residual), residual.size)
    near = squares + swap(squares, other_core)
    squares = near + (swap(squares, other_chip) + swap(squares, diagonal))
    mean_square = squares[:, :1] / D
    scaled = summed * lax.rsqrt(mean_square + 1e-05) * norm_gain.astype(F32)[None, :]
    return (summed.astype(BF16), scaled.astype(BF16))


def solution(mesh):
    split = Mesh(mesh.devices.reshape(SIZES), AXES)
    return jax.shard_map(
        body,
        mesh=split,
        in_specs=(P(COL, TP), P(COL, TP), P(TP, COL), P(TP, COL), P(COL)),
        out_specs=(P(TP, COL), P(TP, COL)),
        check_vma=False,
    )
```
